32 devices in a mesh: gx: 2 (over y), gy: 4 (over z), gz: 4 (over x, core).
Axes of the slice: x: 2, y: 2, z: 4, core: 2. Of those that a mesh axis runs over, the one named last changes fastest.
Arguments:
- node_latent: bfloat16 [2, 4, 4, 512, 128], P('gx', 'gy', 'gz'), may hold values from -6 to 6
- ghost_latent: bfloat16 [2, 4, 4, 6, 64, 128], P('gx', 'gy', 'gz'), may hold values from -6 to 6
- edge_latent: bfloat16 [2, 4, 4, 2816, 128], P('gx', 'gy', 'gz'), may hold values from -6 to 6
- senders: int32 [2, 4, 4, 2816], P('gx', 'gy', 'gz'), may hold values from 0 to 895
- receivers: int32 [2, 4, 4, 2816], P('gx', 'gy', 'gz'), may hold values from 0 to 511, never falling along the last dimension, each value on 1 to 12 neighbouring positions
- export_rows: int32 [2, 4, 4, 6, 64], P('gx', 'gy', 'gz'), may hold values from 0 to 512, as said below
- node_cotangent: bfloat16 [2, 4, 4, 512, 128], P('gx', 'gy', 'gz'), may hold values from -6 to 6
- edge_cotangent: bfloat16 [2, 4, 4, 2816, 128], P('gx', 'gy', 'gz'), may hold values from -6 to 6
- w_edge_in: bfloat16 [384, 128], replicated, may hold values from -0.3125 to 0.3125
- w_edge_hidden: bfloat16 [2, 128, 128], replicated, may hold values from -0.5 to 0.5
- b_edge: float32 [3, 128], replicated, may hold values from -3 to 3
- gain_edge: float32 [128], replicated, may hold values from 0.1 to 1.9
- shift_edge: float32 [128], replicated, may hold values from -3 to 3
- w_node_in: bfloat16 [256, 128], replicated, may hold values from -0.375 to 0.375
- w_node_hidden: bfloat16 [2, 128, 128], replicated, may hold values from -0.5 to 0.5
- b_node: float32 [3, 128], replicated, may hold values from -3 to 3
- gain_node: float32 [128], replicated, may hold values from 0.1 to 1.9
Outputs:
- node_grad: float32 [2, 4, 4, 512, 128], P('gx', 'gy', 'gz')
- edge_grad: bfloat16 [2, 4, 4, 2816, 128], P('gx', 'gy', 'gz')
- grad_w_edge_in: float32 [384, 128], replicated
- grad_w_edge_hidden: float32 [2, 128, 128], replicated
- grad_b_edge: float32 [3, 128], replicated
- grad_gain_edge: float32 [128], replicated
- grad_shift_edge: float32 [128], replicated
- grad_w_node_in: float32 [256, 128], replicated
- grad_w_node_hidden: float32 [2, 128, 128], replicated
- grad_b_node: float32 [3, 128], replicated
- grad_gain_node: float32 [128], replicated
The draws below stay inside these ranges and needn't reach their ends.
Inputs may be any that keep to these rules, and one draw needn't show every extreme that they name: `export_rows`: for each block and face the leading slots hold distinct owned rows of that block; the remaining slots hold 512, marking an empty slot.
All inputs are finite; a program needn't handle non-finite values.
Results may differ from the reference program's by a relative error of at most 0.02.
Values sent between devices are 32-bit elements; how exact they have to be, the bound alone decides.
No kernel may reach another device: no remote copies, remote signals or barrier semaphores. Data moves between devices by JAX's collectives and lax.ppermute only.
A program may use at most 64 MiB of HBM per device.

```python
import math
import jax
import jax.numpy as jnp
import numpy as np
from jax import lax

D = 128
NODES_PER_BLOCK = 512
GHOST_SLOTS = 64
EDGE_DEV = 2816
NODES = 16384
EDGES = 90112
N_GX = 2
N_GY = 4
N_GZ = 4


def draw_export_rows(key, part):
    slab_count = N_GX * N_GY * N_GZ * 6
    slab_keys = jax.random.split(jax.random.fold_in(key, 11), slab_count)

    def one_slab(slab_key):
        order_key, vacant_random_key = jax.random.split(slab_key)
        picked_slots = jax.random.permutation(order_key, NODES_PER_BLOCK)[:GHOST_SLOTS].astype(jnp.int32)
        vacant_slots = jax.random.randint(vacant_random_key, (), 0, GHOST_SLOTS // 4 + 1, dtype=jnp.int32)
        ghost_positions = jnp.arange(GHOST_SLOTS, dtype=jnp.int32)
        return jnp.where(ghost_positions < GHOST_SLOTS - vacant_slots, picked_slots, NODES_PER_BLOCK).astype(jnp.int32)
    return jax.vmap(one_slab)(slab_keys).reshape(N_GX, N_GY, N_GZ, 6, GHOST_SLOTS)


def set_ends(values, rng, low, top_value):
    longest = values.shape.index(max(values.shape))
    spots = []
    for shift in (0, 1):
        where = [jax.random.randint(jax.random.fold_in(rng, axis), (), 0, length) for axis, length in enumerate(values.shape)]
        where[longest] = (where[longest] + shift) % values.shape[longest]
        spots.append(tuple(where))
    return values.at[spots[0]].set(low).at[spots[1]].set(top_value)


def shard_levels(own_key, extent, cuts, low, largest):
    level = 1.0
    for dim, shards_of in cuts:
        draws = jax.random.uniform(jax.random.fold_in(jax.random.fold_in(own_key, 6), dim), (shards_of,), jnp.float32, low / len(cuts), largest / len(cuts))
        level = level * jnp.repeat(jnp.exp(draws), extent[dim] // shards_of).reshape((-1,) + (1,) * (len(extent) - 1 - dim))
    return level


def split_up(amount, total, limit, slope):
    portions = [(1 << 20) // math.isqrt(standing ** slope) + 1 for standing in range(2, amount + 1)]
    rest, counts = total - limit - (amount - 1), [1] * (amount - 1)
    while rest > 0:
        free = [i for i in range(amount - 1) if counts[i] < limit]
        whole, remaining = sum([portions[i] for i in free]), rest
        for i in free:
            addition = min(limit - counts[i], max(1, remaining * portions[i] // whole), rest)
            counts[i] = counts[i] + addition
            rest = rest - addition
    return np.array([limit] + counts)


def uneven_parts(stream_key, count, total, most, skew):
    if count == 2:
        one = jax.random.randint(stream_key, (), max(1, total - most), min(most, total - 1) + 1)
        return jnp.stack([one, total - one])
    lengths = jnp.asarray(split_up(count, total, most, skew), jnp.int32)
    pairs = (count - 1) // 2
    source_of, receiver = lengths[1:1 + 2 * pairs:2], lengths[2:2 + 2 * pairs:2]
    slack = jnp.minimum(source_of - 1, most - receiver)
    passed = jax.random.randint(jax.random.fold_in(stream_key, 1), (pairs,), 0, 1 << 20) % (slack + 1)
    lengths = lengths.at[1:1 + 2 * pairs:2].set(source_of - passed).at[2:2 + 2 * pairs:2].set(receiver + passed)
    return lengths[jax.random.permutation(jax.random.fold_in(stream_key, 2), count)]


def gaussian(key, dims, scale, bound, cuts=(), kind=jnp.bfloat16):
    result = jax.random.normal(key, dims, jnp.float32) * scale
    if len(cuts) > 0:
        result = shard_levels(key, dims, cuts, -0.22, 0.18) * result
    return jnp.clip(result, min=-bound, max=bound).astype(kind)


def setup_inputs(seed: int = 0) -> dict:
    key_of = jax.random.split(jax.random.key(seed), 18)
    node_latent = gaussian(key_of[0], (N_GX, N_GY, N_GZ, NODES_PER_BLOCK, D), 1.0, 6.0, ((0, 2), (1, 4), (2, 4)))
    ghost_latent = gaussian(key_of[1], (N_GX, N_GY, N_GZ, 6, GHOST_SLOTS, D), 1.0, 6.0, ((0, 2), (1, 4), (2, 4)))
    edge_latent = gaussian(key_of[2], (N_GX, N_GY, N_GZ, EDGE_DEV, D), 1.0, 6.0, ((0, 2), (1, 4), (2, 4)))
    senders = set_ends(jax.random.randint(key_of[3], (N_GX, N_GY, N_GZ, EDGE_DEV), 0, NODES_PER_BLOCK + 6 * GHOST_SLOTS), jax.random.fold_in(key_of[3], 1), 0, (NODES_PER_BLOCK + 6 * GHOST_SLOTS) - 1).astype(jnp.int32)
    receivers = jax.vmap(lambda own: jnp.searchsorted(jnp.cumsum(uneven_parts(own, NODES_PER_BLOCK, EDGE_DEV, 12, 1)), jnp.arange(EDGE_DEV), side="right"))(jax.random.split(key_of[4], N_GX * N_GY * N_GZ)).reshape((N_GX, N_GY, N_GZ, EDGE_DEV)).astype(jnp.int32)
    export_rows = draw_export_rows(jax.random.fold_in(key_of[17], 71), 0)
    node_cotangent = gaussian(key_of[6], (N_GX, N_GY, N_GZ, NODES_PER_BLOCK, D), 1.0, 6.0, ((0, 2), (1, 4), (2, 4)))
    edge_cotangent = gaussian(key_of[7], (N_GX, N_GY, N_GZ, EDGE_DEV, D), 1.0, 6.0, ((0, 2), (1, 4), (2, 4)))
    w_edge_in = gaussian(key_of[8], (3 * D, D), (3 * D) ** -0.5, 0.3125)
    w_edge_hidden = gaussian(key_of[9], (2, D, D), D ** -0.5, 0.5)
    b_edge = gaussian(key_of[10], (3, D), 0.5, 3.0, (), jnp.float32)
    gain_edge = jnp.clip(1.0 + 0.18 * jax.random.normal(key_of[11], (D,), jnp.float32), 0.1, 1.9)
    shift_edge = gaussian(key_of[12], (D,), 0.5, 3.0, (), jnp.float32)
    w_node_in = gaussian(key_of[13], (2 * D, D), (2 * D) ** -0.5, 0.375)
    w_node_hidden = gaussian(key_of[14], (2, D, D), D ** -0.5, 0.5)
    b_node = gaussian(key_of[15], (3, D), 0.5, 3.0, (), jnp.float32)
    gain_node = jnp.clip(1.0 + 0.18 * jax.random.normal(key_of[16], (D,), jnp.float32), 0.1, 1.9)
    return dict(node_latent=node_latent, ghost_latent=ghost_latent, edge_latent=edge_latent, senders=senders, receivers=receivers, export_rows=export_rows, node_cotangent=node_cotangent, edge_cotangent=edge_cotangent, w_edge_in=w_edge_in, w_edge_hidden=w_edge_hidden, b_edge=b_edge, gain_edge=gain_edge, shift_edge=shift_edge, w_node_in=w_node_in, w_node_hidden=w_node_hidden, b_node=b_node, gain_node=gain_node)


EPSILON = 1e-05

def matmul(left, right):
    return jnp.dot(left, right, preferred_element_type=jnp.float32)

def contract_rows(left, right):
    return lax.dot_general(left, right, (((0,), (0,)), ((), ())), preferred_element_type=jnp.float32)

def silu_parts(preact):
    sigmoid = jax.nn.sigmoid(preact)
    return (preact * sigmoid, sigmoid * (1.0 + preact * (1.0 - sigmoid)))

def norm_parts(preact):
    centred = preact - lax.optimization_barrier(jnp.mean(preact, -1, keepdims=True))
    inv_std = lax.rsqrt(lax.optimization_barrier(jnp.mean(centred * centred, -1, keepdims=True)) + EPSILON)
    return (centred * inv_std, inv_std)

def norm_back(grad_out, gain, normed, inv_std):
    scaled = grad_out * gain
    return inv_std * (scaled - lax.optimization_barrier(jnp.mean(scaled, -1, keepdims=True)) - normed * lax.optimization_barrier(jnp.mean(scaled * normed, -1, keepdims=True)))

def mlp_forward(inputs, w_first, w_hidden, biases):
    first_pre = matmul(inputs, w_first) + biases[0]
    first_act, first_slope = silu_parts(first_pre)
    first_out = first_act.astype(jnp.bfloat16)
    second_pre = matmul(first_out, w_hidden[0]) + biases[1]
    second_act, second_slope = silu_parts(second_pre)
    second_out = second_act.astype(jnp.bfloat16)
    final_pre = matmul(second_out, w_hidden[1]) + biases[2]
    return ((first_out, second_out, first_slope, second_slope), final_pre)

def mlp_back_inputs(final_grad, saved, w_first, w_hidden):
    first_out, second_out, first_slope, second_slope = saved
    final_round = final_grad.astype(jnp.bfloat16)
    second_grad = matmul(final_round, w_hidden[1].T) * second_slope
    second_round = second_grad.astype(jnp.bfloat16)
    first_grad = matmul(second_round, w_hidden[0].T) * first_slope
    first_round = first_grad.astype(jnp.bfloat16)
    input_grad = matmul(first_round, w_first.T)
    bias_grad = jnp.stack([lax.optimization_barrier(jnp.sum(first_grad, 0)), lax.optimization_barrier(jnp.sum(second_grad, 0)), lax.optimization_barrier(jnp.sum(final_grad, 0))])
    return ((first_round, second_round, final_round), bias_grad, input_grad)

def mlp_back_weights(inputs, saved, rounded):
    first_weight = contract_rows(inputs, rounded[0])
    hidden_weight = jnp.stack([contract_rows(saved[0], rounded[1]), contract_rows(saved[1], rounded[2])])
    return (first_weight, hidden_weight)

def forward_states(node_rows, ghost_rows, edge_rows, sender_ids, receiver_ids, params):
    node_count, feature_width = node_rows.shape
    full_rows = jnp.concatenate([node_rows, ghost_rows.reshape(-1, feature_width)], 0)
    edge_inputs = jnp.concatenate([edge_rows, full_rows[sender_ids], full_rows[receiver_ids]], 1)
    edge_stored_state, edge_pre = mlp_forward(edge_inputs, params[0], params[1], params[2])
    edge_normed, edge_inv = norm_parts(edge_pre)
    edge_new = (edge_normed * params[3] + params[4]).astype(jnp.bfloat16)
    aggregate = jax.ops.segment_sum(edge_new.astype(jnp.float32), receiver_ids, num_segments=node_count).astype(jnp.bfloat16)
    node_input_rows = jnp.concatenate([node_rows, aggregate], 1)
    node_saved, node_pre = mlp_forward(node_input_rows, params[5], params[6], params[7])
    node_normed, node_inv = norm_parts(node_pre)
    return ((edge_inputs, edge_stored_state, edge_normed, edge_inv), (node_input_rows, node_saved, node_normed, node_inv))

def node_backward(node_state, node_cot, params):
    node_input_rows, node_saved, node_normed, node_inv = node_state
    upstream = node_cot.astype(jnp.float32)
    gain_grad = lax.optimization_barrier(jnp.sum(upstream * node_normed, 0))
    final_grad = norm_back(upstream, params[8], node_normed, node_inv)
    rounded, bias_grad, input_grad = mlp_back_inputs(final_grad, node_saved, params[5], params[6])
    first_weight, hidden_weight = mlp_back_weights(node_input_rows, node_saved, rounded)
    return (input_grad, (first_weight, hidden_weight, bias_grad, gain_grad))

def edge_backward_inputs(edge_state, edge_cot, agg_grad, sender_ids, receiver_ids, total_rows, params):
    edge_inputs, edge_stored_state, edge_normed, edge_inv = edge_state
    feature_width = edge_cot.shape[1]
    edge_upstream = edge_cot.astype(jnp.float32)
    new_grad = edge_upstream + agg_grad[receiver_ids]
    gain_grad = lax.optimization_barrier(jnp.sum(new_grad * edge_normed, 0))
    shift_grad = lax.optimization_barrier(jnp.sum(new_grad, 0))
    final_grad = norm_back(new_grad, params[3], edge_normed, edge_inv)
    rounded, bias_grad, input_grad = mlp_back_inputs(final_grad, edge_stored_state, params[0], params[1])
    edge_grad = (edge_upstream + input_grad[:, :feature_width]).astype(jnp.bfloat16)
    full_grad = jax.ops.segment_sum(input_grad[:, feature_width:2 * feature_width], sender_ids, num_segments=total_rows)
    full_grad = full_grad + jax.ops.segment_sum(input_grad[:, 2 * feature_width:], receiver_ids, num_segments=total_rows)
    return (edge_grad, full_grad, rounded, (bias_grad, gain_grad, shift_grad))

def block_pass(node_rows, ghost_rows, edge_rows, sender_ids, receiver_ids, node_cot, edge_cot, params):
    node_count, feature_width = node_rows.shape
    total_rows = node_count + ghost_rows.shape[0] * ghost_rows.shape[1]
    edge_state, node_state = forward_states(node_rows, ghost_rows, edge_rows, sender_ids, receiver_ids, params)
    node_input_grad, node_weights = node_backward(node_state, node_cot, params)
    edge_grad, full_grad, rounded, edge_small = edge_backward_inputs(edge_state, edge_cot, node_input_grad[:, feature_width:], sender_ids, receiver_ids, total_rows, params)
    first_weight, hidden_weight = mlp_back_weights(edge_state[0], edge_state[1], rounded)
    local_grad = node_cot.astype(jnp.float32) + node_input_grad[:, :feature_width] + full_grad[:node_count]
    ghost_grad = full_grad[node_count:].reshape(ghost_rows.shape)
    weights = (first_weight, hidden_weight) + edge_small + node_weights
    return (local_grad, ghost_grad, edge_grad, weights)

def add_rows(target, rows, values):
    return target.at[rows].add(values, mode='drop')

def reference(node_latent, ghost_latent, edge_latent, senders, receivers, export_rows, node_cotangent, edge_cotangent, w_edge_in, w_edge_hidden, b_edge, gain_edge, shift_edge, w_node_in, w_node_hidden, b_node, gain_node):
    params = (w_edge_in, w_edge_hidden, b_edge, gain_edge, shift_edge, w_node_in, w_node_hidden, b_node, gain_node)
    block_count = N_GX * N_GY * N_GZ
    grid_shape = (N_GX, N_GY, N_GZ)

    def flatten(array):
        return array.reshape((block_count,) + array.shape[3:])
    stacked = tuple((flatten(array) for array in (node_latent, ghost_latent, edge_latent, senders, receivers, node_cotangent, edge_cotangent)))

    def visit(running, block_item):
        local_grad, ghost_grad, edge_grad, weights = block_pass(*block_item, params)
        return (tuple((total + term for total, term in zip(running, weights))), (local_grad, ghost_grad, edge_grad))
    start = tuple((jnp.zeros(param.shape, jnp.float32) for param in params))
    totals, (local_all, ghost_all, edge_all) = lax.scan(visit, start, stacked)
    ghost_grid = ghost_all.reshape(grid_shape + ghost_all.shape[1:])
    rows_flat = flatten(export_rows)
    node_grad = local_all
    for face_index in range(6):
        incoming = jnp.roll(ghost_grid[:, :, :, face_index], 1 - 2 * (face_index % 2), face_index // 2)
        node_grad = jax.vmap(add_rows)(node_grad, rows_flat[:, face_index], flatten(incoming))
    node_grad = node_grad.reshape(grid_shape + node_grad.shape[1:])
    edge_grad = edge_all.reshape(grid_shape + edge_all.shape[1:])
    edge_scale = EDGES ** (-0.5)
    node_scale = NODES ** (-0.5)
    return (node_grad, edge_grad, totals[0] * edge_scale, totals[1] * edge_scale, totals[2] * edge_scale, totals[3] * edge_scale, totals[4] * edge_scale, totals[5] * node_scale, totals[6] * node_scale, totals[7] * node_scale, totals[8] * node_scale)
```

```python
import jax
import jax.numpy as jnp
from jax import lax
from jax.experimental import pallas as pl
from jax.experimental.pallas import tpu as pltpu
from jax.sharding import PartitionSpec as P

EPSILON = 1e-05
AXES = ("gx", "gy", "gz")
BF16 = jnp.bfloat16
F32 = jnp.float32


def from_behind(x, axis, by):
    peers = lax.axis_size(axis)
    return lax.ppermute(x, axis, [(i, (i + by) % peers) for i in range(peers)])


def dot(left, right):
    return jnp.dot(left, right, preferred_element_type=F32)


def dot_t(left, right):
    return lax.dot_general(left, right, (((1,), (1,)), ((), ())), preferred_element_type=F32)


def dot_rows(left, right):
    return lax.dot_general(left, right, (((0,), (0,)), ((), ())), preferred_element_type=F32)


def hi_lo(x):
    high = x.astype(BF16)
    return high, (x - high.astype(F32)).astype(BF16)


def fold_halves(x):
    half = x.shape[1] // 2
    return x[:, :half] + x[:, half:]


def silu_parts(preact):
    sigmoid = 1.0 / (1.0 + jnp.exp(-preact))
    act = preact * sigmoid
    return act.astype(BF16), sigmoid + act * (1.0 - sigmoid)


def norm_parts(preact):
    centred = preact - jnp.mean(preact, -1, keepdims=True)
    inv_std = lax.rsqrt(jnp.mean(centred * centred, -1, keepdims=True) + EPSILON)
    return centred * inv_std, inv_std


def norm_back(grad_out, gain, normed, inv_std):
    scaled = grad_out * gain
    return inv_std * (
        scaled
        - jnp.mean(scaled, -1, keepdims=True)
        - normed * jnp.mean(scaled * normed, -1, keepdims=True)
    )


def rows8(x):
    return jnp.sum(x.reshape(x.shape[0] // 8, 8, x.shape[1]), 0)


def total(x):
    return jnp.sum(x, 0, keepdims=True)


def pick_chunk(rows):
    for size in (256, 128):
        if rows % size == 0:
            return size
    return rows


def block_kernel(edge_scale, node_scale, chunk):
    def kernel(
        node_ref,
        ghost_ref,
        edge_ref,
        snd_ref,
        rcv_ref,
        ncot_ref,
        ecot_ref,
        w1_ref,
        wh_ref,
        b_ref,
        gain_ref,
        shift_ref,
        nw1_ref,
        nwh_ref,
        nb_ref,
        ngain_ref,
        local_ref,
        ghost_out_ref,
        edge_out_ref,
        grads_ref,
        one_ref,
        one_t_ref,
        table_ref,
        z1_ref,
        z2_ref,
        s1_ref,
        s2_ref,
        n_ref,
        inv_ref,
        g1_ref,
        g2_ref,
        g3_ref,
        new_ref,
        small_ref,
    ):
        nodes, width = node_ref.shape
        ghosts = ghost_ref.shape[0]
        full_count = nodes + ghosts
        total_rows = full_count + nodes
        edges = edge_ref.shape[0]
        steps = edges // chunk
        node = node_ref[...]
        ghost = ghost_ref[...]
        w_edge = w1_ref[0:width, :]
        w_snd = w1_ref[width : 2 * width, :]
        w_rcv = w1_ref[2 * width : 3 * width, :]

        def put_table(first, value):
            high, low = hi_lo(value)
            table_ref[first : first + value.shape[0], 0:width] = high
            table_ref[first : first + value.shape[0], width : 2 * width] = low

        put_table(0, dot(node, w_snd))
        put_table(nodes, dot(ghost, w_snd))
        put_table(full_count, dot(node, w_rcv))
        small_ref[...] = jnp.zeros(small_ref.shape, F32)

        lane = lax.broadcasted_iota(jnp.int32, (chunk, width), 1)
        sub = lax.broadcasted_iota(jnp.int32, (width, chunk), 0)

        def forward(step, carry):
            start = pl.multiple_of(step * chunk, chunk)
            rows = pl.ds(start, chunk)
            snd = jnp.broadcast_to(snd_ref[:, rows], (width, chunk))
            rcv = jnp.broadcast_to(rcv_ref[:, rows], (width, chunk))
            snd_col = snd.T
            rcv_col = rcv.T
            for base in range(0, total_rows, width):
                ids, ids_col, shift = (
                    (snd, snd_col, base) if base < full_count else (rcv, rcv_col, base - full_count)
                )
                one_t_ref[base : base + width, rows] = jnp.where(
                    sub == ids - shift, 1.0, 0.0
                ).astype(BF16)
                one_ref[rows, base : base + width] = jnp.where(
                    lane == ids_col - shift, 1.0, 0.0
                ).astype(BF16)
            pre = fold_halves(dot(one_ref[rows, :], table_ref[...]))
            pre = pre + dot(edge_ref[rows, :], w_edge) + b_ref[0:1, :]
            z1, slope1 = silu_parts(pre)
            z1_ref[rows, :] = z1
            s1_ref[rows, :] = slope1
            z2, slope2 = silu_parts(dot(z1, wh_ref[0]) + b_ref[1:2, :])
            z2_ref[rows, :] = z2
            s2_ref[rows, :] = slope2
            normed, inv = norm_parts(dot(z2, wh_ref[1]) + b_ref[2:3, :])
            n_ref[rows, :] = normed
            inv_ref[rows, :] = jnp.broadcast_to(inv, (chunk, width))
            new_ref[rows, :] = (normed * gain_ref[...] + shift_ref[...]).astype(BF16)
            return carry

        lax.fori_loop(0, steps, forward, 0)

        agg = dot(one_t_ref[full_count:, :], new_ref[...]).astype(BF16)
        pre = dot(node, nw1_ref[0:width, :]) + dot(agg, nw1_ref[width:, :]) + nb_ref[0:1, :]
        nz1, ns1 = silu_parts(pre)
        nz2, ns2 = silu_parts(dot(nz1, nwh_ref[0]) + nb_ref[1:2, :])
        normed, inv = norm_parts(dot(nz2, nwh_ref[1]) + nb_ref[2:3, :])
        upstream = ncot_ref[...].astype(F32)
        node_gain = total(upstream * normed)
        grad3 = norm_back(upstream, ngain_ref[...], normed, inv)
        round3 = grad3.astype(BF16)
        grad2 = dot_t(round3, nwh_ref[1]) * ns2
        round2 = grad2.astype(BF16)
        grad1 = dot_t(round2, nwh_ref[0]) * ns1
        round1 = grad1.astype(BF16)
        local_ref[...] = upstream + dot_t(round1, nw1_ref[0:width, :])
        put_table(full_count, dot_t(round1, nw1_ref[width:, :]))

        base = 5 * width
        grads_ref[base : base + width, :] = dot_rows(node, round1) * node_scale
        grads_ref[base + width : base + 2 * width, :] = dot_rows(agg, round1) * node_scale
        grads_ref[base + 2 * width : base + 3 * width, :] = dot_rows(nz1, round2) * node_scale
        grads_ref[base + 3 * width : base + 4 * width, :] = dot_rows(nz2, round3) * node_scale

        def backward(step, carry):
            start = pl.multiple_of(step * chunk, chunk)
            rows = pl.ds(start, chunk)
            upstream = ecot_ref[rows, :].astype(F32)
            gathered = dot(one_ref[rows, full_count:], table_ref[full_count:, :])
            new_grad = upstream + fold_halves(gathered)
            normed = n_ref[rows, :]
            small_ref[3] += rows8(new_grad * normed)
            small_ref[4] += rows8(new_grad)
            grad3 = norm_back(new_grad, gain_ref[...], normed, inv_ref[rows, :])
            round3 = grad3.astype(BF16)
            g3_ref[rows, :] = round3
            small_ref[2] += rows8(grad3)
            grad2 = dot_t(round3, wh_ref[1]) * s2_ref[rows, :]
            round2 = grad2.astype(BF16)
            g2_ref[rows, :] = round2
            small_ref[1] += rows8(grad2)
            grad1 = dot_t(round2, wh_ref[0]) * s1_ref[rows, :]
            round1 = grad1.astype(BF16)
            g1_ref[rows, :] = round1
            small_ref[0] += rows8(grad1)
            edge_out_ref[rows, :] = (upstream + dot_t(round1, w_edge)).astype(BF16)
            return carry

        lax.fori_loop(0, steps, backward, 0)

        spread = dot(one_t_ref[...], g1_ref[...])
        high, low = hi_lo(spread)
        pairs = jnp.concatenate([high, low], 1)
        snd_pair = jnp.concatenate([w_snd, w_snd], 1)
        rcv_pair = jnp.concatenate([w_rcv, w_rcv], 1)
        local_ref[...] += dot_t(pairs[:nodes], snd_pair) + dot_t(pairs[full_count:], rcv_pair)
        ghost_out_ref[...] = dot_t(pairs[nodes:full_count], snd_pair)

        grads_ref[0:width, :] = dot_rows(edge_ref[...], g1_ref[...]) * edge_scale
        snd_grad = dot_rows(node, pairs[:nodes]) + dot_rows(ghost, pairs[nodes:full_count])
        grads_ref[width : 2 * width, :] = fold_halves(snd_grad) * edge_scale
        grads_ref[2 * width : 3 * width, :] = (
            fold_halves(dot_rows(node, pairs[full_count:])) * edge_scale
        )
        grads_ref[3 * width : 4 * width, :] = dot_rows(z1_ref[...], g2_ref[...]) * edge_scale
        grads_ref[4 * width : 5 * width, :] = dot_rows(z2_ref[...], g3_ref[...]) * edge_scale

        base = 9 * width
        grads_ref[base:, :] = jnp.zeros((grads_ref.shape[0] - base, width), F32)
        for index in range(5):
            grads_ref[base + index : base + index + 1, :] = total(small_ref[index]) * edge_scale
        node_small = (total(grad1), total(grad2), total(grad3), node_gain)
        for index, term in enumerate(node_small):
            grads_ref[base + 5 + index : base + 6 + index, :] = term * node_scale

    return kernel


def finish_kernel(
    local_ref,
    rows_ref,
    r0_ref,
    r1_ref,
    r2_ref,
    r3_ref,
    r4_ref,
    r5_ref,
    sums_ref,
    node_ref,
    w1_ref,
    wh_ref,
    b_ref,
    gain_ref,
    shift_ref,
    nw1_ref,
    nwh_ref,
    nb_ref,
    ngain_ref,
):
    nodes, width = local_ref.shape
    slots = rows_ref.shape[1]
    sub = lax.broadcasted_iota(jnp.int32, (nodes, slots), 0)
    added = jnp.zeros((nodes, 2 * width), F32)
    for face, ref in enumerate((r0_ref, r1_ref, r2_ref, r3_ref, r4_ref, r5_ref)):
        spots = jnp.where(sub == rows_ref[face : face + 1, :], 1.0, 0.0).astype(BF16)
        added = added + dot(spots, jnp.concatenate(hi_lo(ref[...]), 1))
    node_ref[...] = local_ref[...] + fold_halves(added)
    w1_ref[...] = sums_ref[0 : 3 * width, :]
    wh_ref[0] = sums_ref[3 * width : 4 * width, :]
    wh_ref[1] = sums_ref[4 * width : 5 * width, :]
    nw1_ref[...] = sums_ref[5 * width : 7 * width, :]
    nwh_ref[0] = sums_ref[7 * width : 8 * width, :]
    nwh_ref[1] = sums_ref[8 * width : 9 * width, :]
    base = 9 * width
    b_ref[...] = sums_ref[base : base + 3, :]
    gain_ref[...] = sums_ref[base + 3 : base + 4, :]
    shift_ref[...] = sums_ref[base + 4 : base + 5, :]
    nb_ref[...] = sums_ref[base + 5 : base + 8, :]
    ngain_ref[...] = sums_ref[base + 8 : base + 9, :]


def partner(x, axis, mask):
    return lax.ppermute(x, axis, [(i, i ^ mask) for i in range(lax.axis_size(axis))])


def masks_of(axis, reach):
    size = lax.axis_size(axis)
    if size & (size - 1):
        return None
    return [reach * 2**bit - (reach - 1) for bit in range(size.bit_length() - 1)]


def sum_blocks(x):
    halved = masks_of("gz", 1)
    if halved is None:
        return lax.psum(x, AXES)
    side = lax.axis_index("gz")
    for mask in halved:
        half = x.shape[0] // 2
        upper = (side & mask) != 0
        first, second = x[:half], x[half:]
        kept = jnp.where(upper, second, first)
        x = kept + partner(jnp.where(upper, first, second), "gz", mask)
    for axis in ("gx", "gy"):
        masks = masks_of(axis, 2)
        if masks is None:
            x = lax.psum(x, axis)
            continue
        for mask in masks:
            x = x + partner(x, axis, mask)
    for mask in reversed(halved):
        other = partner(x, "gz", mask)
        upper = (side & mask) != 0
        x = jnp.where(upper, jnp.concatenate([other, x]), jnp.concatenate([x, other]))
    return x


def on_device(
    node_latent,
    ghost_latent,
    edge_latent,
    senders,
    receivers,
    export_rows,
    node_cotangent,
    edge_cotangent,
    w_edge_in,
    w_edge_hidden,
    b_edge,
    gain_edge,
    shift_edge,
    w_node_in,
    w_node_hidden,
    b_node,
    gain_node,
):
    nodes, width = node_latent.shape[3:]
    edges = edge_latent.shape[3]
    faces, slots = export_rows.shape[3:]
    ghosts = faces * slots
    devices = 1
    for axis in AXES:
        devices *= lax.axis_size(axis)
    unit = 8 * lax.axis_size("gz")
    grad_rows = -(-(9 * width + 9) // unit) * unit
    chunk = pick_chunk(edges)
    total_rows = 2 * nodes + ghosts

    local, ghost_grad, edge_grad, grads = pl.pallas_call(
        block_kernel(
            float(edges * devices) ** (-0.5), float(nodes * devices) ** (-0.5), chunk
        ),
        out_shape=(
            jax.ShapeDtypeStruct((nodes, width), F32),
            jax.ShapeDtypeStruct((ghosts, width), F32),
            jax.ShapeDtypeStruct((edges, width), BF16),
            jax.ShapeDtypeStruct((grad_rows, width), F32),
        ),
        scratch_shapes=[
            pltpu.VMEM((edges, total_rows), BF16),
            pltpu.VMEM((total_rows, edges), BF16),
            pltpu.VMEM((total_rows, 2 * width), BF16),
            pltpu.VMEM((edges, width), BF16),
            pltpu.VMEM((edges, width), BF16),
            pltpu.VMEM((edges, width), F32),
            pltpu.VMEM((edges, width), F32),
            pltpu.VMEM((edges, width), F32),
            pltpu.VMEM((edges, width), F32),
            pltpu.VMEM((edges, width), BF16),
            pltpu.VMEM((edges, width), BF16),
            pltpu.VMEM((edges, width), BF16),
            pltpu.VMEM((edges, width), BF16),
            pltpu.VMEM((5, 8, width), F32),
        ],
        name="block_pass",
    )(
        node_latent.reshape(nodes, width),
        ghost_latent.reshape(ghosts, width),
        edge_latent.reshape(edges, width),
        senders.reshape(1, edges),
        receivers.reshape(1, edges),
        node_cotangent.reshape(nodes, width),
        edge_cotangent.reshape(edges, width),
        w_edge_in,
        w_edge_hidden,
        b_edge,
        gain_edge.reshape(1, width),
        shift_edge.reshape(1, width),
        w_node_in,
        w_node_hidden,
        b_node,
        gain_node.reshape(1, width),
    )

    returned = []
    for face in range(faces):
        slab = ghost_grad[face * slots : (face + 1) * slots]
        returned.append(from_behind(slab, AXES[face // 2], 1 - 2 * (face % 2)))
    sums = sum_blocks(grads)

    outs = pl.pallas_call(
        finish_kernel,
        out_shape=(
            jax.ShapeDtypeStruct((nodes, width), F32),
            jax.ShapeDtypeStruct((3 * width, width), F32),
            jax.ShapeDtypeStruct((2, width, width), F32),
            jax.ShapeDtypeStruct((3, width), F32),
            jax.ShapeDtypeStruct((1, width), F32),
            jax.ShapeDtypeStruct((1, width), F32),
            jax.ShapeDtypeStruct((2 * width, width), F32),
            jax.ShapeDtypeStruct((2, width, width), F32),
            jax.ShapeDtypeStruct((3, width), F32),
            jax.ShapeDtypeStruct((1, width), F32),
        ),
        name="finish",
    )(local, export_rows.reshape(faces, slots), *returned, sums)
    return (
        outs[0].reshape(node_latent.shape),
        edge_grad.reshape(edge_latent.shape),
        outs[1],
        outs[2],
        outs[3],
        outs[4].reshape(width),
        outs[5].reshape(width),
        outs[6],
        outs[7],
        outs[8],
        outs[9].reshape(width),
    )


def solution(mesh):
    block = P("gx", "gy", "gz")
    return jax.shard_map(
        on_device,
        mesh=mesh,
        in_specs=(block,) * 8 + (P(),) * 9,
        out_specs=(block, block) + (P(),) * 9,
        check_vma=False,
    )
```
